128 devices in a mesh: ops: 64 (over y, x, z), blk: 2 (over core).
Axes of the slice: x: 4, y: 4, z: 4, core: 2. Of those that a mesh axis runs over, the one named last changes fastest.
Arguments:
- operators_left: bfloat16 [4096, 256, 256], P('ops', None, 'blk'), may hold values from -16 to 16
- operators_right: bfloat16 [4096, 256, 256], P('ops'), may hold values from -0.00036621094 to 0.00036621094
- wavefunction: bfloat16 [256, 3, 256], P('blk', None, 'ops'), may hold values from -6 to 6
- rotation: bfloat16 [256, 128], replicated, may hold values from -0.375 to 0.375
- pair_count: int32 [64], P('ops'), may hold values from 16 to 64, as said below
- next_owner: int32 [4096, 1], P('ops'), may hold values from 0 to 63; in each aligned block of 64 rows (0 to 63, 64 to 127, ...) at most 2 rows name the same one
Outputs:
- sigma: float32 [256, 3, 256], P(('ops', 'blk'))
- renewed: bfloat16 [64, 128, 128, 128], P('ops', None, 'blk')
The draws below stay inside these ranges and needn't reach their ends.
Inputs may be any that keep to these rules, and one draw needn't show every extreme that they name: Each owner's live pairs fill its first pair_count slots; at least one owner has all 64 slots live. `next_owner`: among the 64 slots of one owner, at most 2 name the same next owner.
All inputs are finite; a program needn't handle non-finite values.
Results may differ from the reference program's by a relative error of at most 0.0073.
Values may be sent and summed in bfloat16 or wider, within the bound.
No kernel may reach another device: no remote copies, remote signals or barrier semaphores. Data moves between devices by JAX's collectives and lax.ppermute only.
A program may use at most 128 MiB of HBM per device.

```python
import math
import jax
import jax.numpy as jnp
import numpy as np
from jax import lax

L = 256
R = 256
K = 128
NV = 3
SLOTS = 64
PAIRS = 4096
CAP = 2
INBOX = 128
N_OPS = 64


def draw_pair_count(key, part):
    owners = PAIRS // SLOTS
    counts = jax.random.randint(jax.random.fold_in(key, 11), (owners,), SLOTS // 4, 3 * SLOTS // 4 + 1, dtype=jnp.int32)
    fullest = jax.random.randint(jax.random.fold_in(key, 12), (), 0, owners, dtype=jnp.int32)
    return jnp.where(jnp.arange(owners, dtype=jnp.int32) == fullest, SLOTS, counts).astype(jnp.int32)


def spiked(entries, stream_key, source, target, blocks, factor):
    owner, partner = [(jnp.arange(entries.shape[axis_at]) // (entries.shape[axis_at] // blocks)).reshape([-1 if axis == axis_at else 1 for axis in range(entries.ndim)]) for axis_at in (source, target)]
    chosen = jax.random.permutation(stream_key, blocks)[partner]
    strong = (owner == chosen) | (owner == (partner + blocks // 2) % blocks)
    return jnp.where(strong, factor * entries, entries)


def steps_of(own_key, shape, shards, least, high):
    loudness, own = 1.0, jax.random.fold_in(own_key, 6)
    for position, blocks in shards:
        heights = jnp.exp(jax.random.uniform(jax.random.fold_in(own, position), (blocks,), jnp.float32, least / len(shards), high / len(shards)))
        loudness = loudness * jnp.repeat(heights, shape[position] // blocks).reshape([-1 if axis == position else 1 for axis in range(len(shape))])
    return loudness


def routed_block(own_key, own, number, rows, amount, top, reach, slope):
    order = jax.random.permutation(own_key, amount)
    crowded, common = load_shares(amount, rows * top, reach, slope, True), load_shares(amount, rows * top, reach, slope, False)
    places = jnp.arange(amount)

    def named(tallies, offset_by):
        used = int((tallies > 0).sum())
        fixed = max(1, used // 4)
        passed = fixed + (places - fixed + offset_by * (used - fixed)) % max(1, amount - fixed)
        return jnp.zeros((amount,), jnp.int32).at[order[jnp.where(places < fixed, places, passed)]].set(jnp.asarray(tallies, jnp.int32))

    tallies = jnp.where(number % 4 == 0, named(crowded, number // 4), named(common, number - number // 4 - 1))
    mixed = jax.random.permutation(jax.random.fold_in(own, 3), amount)
    source_of, receiver = mixed[0:amount // 2 * 2:2], mixed[1:amount // 2 * 2:2]
    room = jnp.minimum(tallies[source_of] - 1, reach - tallies[receiver]) // 2
    room = jnp.where((source_of == order[0]) | (receiver == order[0]) | (tallies[receiver] == 0), 0, jnp.maximum(room, 0))
    passed = jax.random.randint(jax.random.fold_in(own, 4), (amount // 2,), 0, 1 << 20) % (room + 1)
    tallies = tallies.at[source_of].add(-passed).at[receiver].add(passed)
    items = jnp.searchsorted(jnp.cumsum(tallies), jnp.arange(rows * top), side="right").astype(jnp.int32)
    grid = items.reshape(top, rows).T
    grid = grid[jax.random.permutation(jax.random.fold_in(own, 1), rows)]
    offset_by = jax.random.randint(jax.random.fold_in(own, 2), (rows, 1), 0, top)
    return jnp.take_along_axis(grid, (jnp.arange(top)[None, :] + offset_by) % top, axis=1)


def load_shares(amount, total, most, slope, full):
    weights = [(1 << 20) // math.isqrt(standing ** slope) + 1 for standing in range(1, amount + 1)]
    largest = most if full else min(most, max(-(-total // amount), total * weights[0] // sum(weights)))
    least = 1 if total - largest >= amount - 1 else 0
    given, spare = [largest] + [least] * (amount - 1), total - largest - least * (amount - 1)
    while spare > 0:
        free = [i for i in range(1, amount) if given[i] < largest] or [i for i in range(1, amount) if given[i] < most]
        pool, budget = sum([weights[i] for i in free]), spare
        for i in free:
            addition = min(most - given[i], max(1, budget * weights[i] // pool), spare)
            given[i] = given[i] + addition
            spare = spare - addition
    return np.array(given)


def centred(key, extent, scale, bound, shards=(), kind=jnp.bfloat16):
    drawn = jax.random.normal(key, extent, jnp.float32) * scale
    if len(shards) > 0:
        drawn = steps_of(key, extent, shards, -0.22, 0.18) * drawn
    return jnp.clip(drawn, min=-bound, max=bound).astype(kind)


def gaussian_with(own_key, dims, deviation, most, pieces, heavy, kind=jnp.bfloat16):
    array = deviation * jax.random.normal(own_key, dims, jnp.float32)
    if pieces:
        array = array * steps_of(own_key, dims, pieces, -0.22, 0.18)
    return jnp.clip(spiked(array, jax.random.fold_in(own_key, 3), *heavy), -most, most).astype(kind)


def setup_inputs(seed: int = 0) -> dict:
    key_of = jax.random.split(jax.random.key(seed), 7)
    operators_left = gaussian_with(key_of[0], (PAIRS, L, L), 1.0, 16.0, ((0, 64), (2, 2)), (0, 1, 64, 4.0))
    operators_right = centred(key_of[1], (PAIRS, R, R), (R * L * PAIRS) ** -0.5, 0.00036621094, ((0, 64),))
    wavefunction = centred(key_of[2], (L, NV, R), 1.0, 6.0, ((0, 2), (2, 64)))
    rotation = centred(key_of[3], (L, K), L ** -0.5, 0.375)
    pair_count = draw_pair_count(jax.random.fold_in(key_of[6], 71), 0)
    next_owner_keys = jax.random.split(jax.random.fold_in(key_of[5], 1), PAIRS // SLOTS)
    next_owner_turns = jax.random.permutation(jax.random.fold_in(key_of[5], 3), PAIRS // SLOTS)
    next_owner = jax.vmap(lambda own, number: routed_block(jax.random.fold_in(key_of[5], 2), own, number, SLOTS, N_OPS, 1, CAP, 2))(next_owner_keys, next_owner_turns).reshape((PAIRS, 1))
    return {"operators_left": operators_left, "operators_right": operators_right, "wavefunction": wavefunction, "rotation": rotation, "pair_count": pair_count, "next_owner": next_owner}


def reference(operators_left, operators_right, wavefunction, rotation, pair_count, next_owner):
    wave_float = wavefunction.astype(jnp.float32)
    rot_float = rotation.astype(jnp.float32)
    left_grouped = operators_left.reshape(N_OPS, SLOTS, L, L)
    right_grouped = operators_right.reshape(N_OPS, SLOTS, R, R)
    owner_targets = next_owner.reshape(N_OPS, SLOTS)

    def owner_work(packed):
        lefts, rights, live_count, targets = packed
        living = jnp.arange(SLOTS, dtype=jnp.int32) < live_count
        lefts_float = lefts.astype(jnp.float32)
        products = jnp.einsum("inr,psr->pins", wave_float, rights.astype(jnp.float32)).astype(jnp.bfloat16)
        products = jnp.where(living[:, None, None, None], products, jnp.zeros_like(products))
        term = jnp.einsum("pij,pjns->ins", lefts_float, products.astype(jnp.float32))
        rotated = jnp.einsum("ik,pij->pkj", rot_float, lefts_float).astype(jnp.bfloat16)
        blocks = jnp.einsum("pkj,jl->pkl", rotated.astype(jnp.float32), rot_float).astype(jnp.bfloat16)
        blocks = jnp.where(living[:, None, None], blocks, jnp.zeros_like(blocks))
        chosen = ((targets[:, None] == jnp.arange(N_OPS, dtype=jnp.int32)[None, :]) & living[:, None]).astype(jnp.int32)
        earlier = jnp.cumsum(chosen, axis=0) - chosen
        ranking = jnp.sum(earlier * chosen, axis=1)
        address = targets * CAP + ranking
        placing = ((address[None, :] == jnp.arange(N_OPS * CAP, dtype=jnp.int32)[:, None]) & living[None, :]).astype(jnp.float32)
        outgoing = jnp.einsum("ap,pkl->akl", placing, blocks.astype(jnp.float32)).astype(jnp.bfloat16)
        return term, outgoing

    terms, sent = lax.map(owner_work, (left_grouped, right_grouped, pair_count, owner_targets))
    sigma = jnp.sum(terms, axis=0)
    renewed = sent.reshape(N_OPS, N_OPS, CAP, K, K).transpose(1, 0, 2, 3, 4).reshape(N_OPS, INBOX, K, K)
    return sigma, renewed
```

```python
import jax
import jax.numpy as jnp
from jax import lax
from jax.experimental import pallas as pl
from jax.experimental.pallas import tpu as pltpu
from jax.sharding import Mesh
from jax.sharding import PartitionSpec as P


OPS = ("ops_0", "ops_1", "ops_2")
ALL = ("ops_0", "ops_1", "ops_2", "blk")
GROUP = 8
MIB = 1 << 20
LANES = 128


def rotate_kernel(side_ref, left_ref, rot_ref, keep_ref, send_ref, lefts, turned, arrived):
    slots, half, width = keep_ref.shape
    groups = slots // GROUP

    def fetch(g):
        part = pl.ds(g * GROUP, GROUP)
        return pltpu.make_async_copy(left_ref.at[part], lefts.at[part], arrived.at[g])

    for g in range(groups):
        fetch(g).start()
    own_low = side_ref[0] == 0
    turned[...] = rot_ref[...].T
    rot = turned[...]
    for g in range(groups):
        fetch(g).wait()
        for p in range(g * GROUP, (g + 1) * GROUP, 2):
            both = jnp.concatenate([lefts[p], lefts[p + 1]], axis=1)
            rotated = jnp.dot(rot, both, preferred_element_type=jnp.float32).astype(jnp.bfloat16)
            low, high = rotated[:half], rotated[half:]
            keep = jnp.where(own_low, low, high)
            send = jnp.where(own_low, high, low)
            for q in range(2):
                keep_ref[p + q] = keep[:, q * width : (q + 1) * width]
                send_ref[p + q] = send[:, q * width : (q + 1) * width]


def rotate_left(side, operators_left, rotation):
    slots, rows, cols = operators_left.shape
    new = rotation.shape[1]
    half = jax.ShapeDtypeStruct((slots, new // 2, cols), jnp.bfloat16)
    vmem = pl.BlockSpec(memory_space=pltpu.VMEM)
    return pl.pallas_call(
        rotate_kernel,
        in_specs=[
            pl.BlockSpec(memory_space=pltpu.SMEM),
            pl.BlockSpec(memory_space=pltpu.HBM),
            vmem,
        ],
        out_specs=[vmem, vmem],
        out_shape=[half, half],
        scratch_shapes=[
            pltpu.VMEM((slots, rows, cols), jnp.bfloat16),
            pltpu.VMEM((new, rows), jnp.bfloat16),
            pltpu.SemaphoreType.DMA((slots // GROUP,)),
        ],
        compiler_params=pltpu.CompilerParams(vmem_limit_bytes=50 * MIB),
        cost_estimate=pl.CostEstimate(
            flops=2 * slots * rows * cols * new,
            bytes_accessed=2 * slots * cols * (rows + new),
            transcendentals=0,
        ),
        name="rotate_left",
    )(side, operators_left, rotation)


def renew_kernel(side_ref, count_ref, place_ref, keep_ref, other_ref, rot_ref, out_ref):
    slots, half, width = keep_ref.shape
    live = count_ref[0]
    own_low = side_ref[0] == 0
    top, bottom = rot_ref[:width], rot_ref[width:]
    rot_own = jnp.where(own_low, top, bottom)
    rot_far = jnp.where(own_low, bottom, top)
    rot = jnp.concatenate([rot_own, rot_far], axis=0)
    out_ref[...] = jnp.zeros_like(out_ref)
    for first in range(slots - GROUP, -1, -GROUP):
        w = jnp.concatenate(
            [keep_ref[first : first + GROUP], other_ref[first : first + GROUP]], axis=2
        ).reshape(GROUP * half, 2 * width)
        b = jnp.dot(w, rot, preferred_element_type=jnp.float32).astype(jnp.bfloat16)
        for q in range(GROUP - 1, -1, -1):
            block = b[q * half : (q + 1) * half]
            alive = first + q < live
            out_ref[jnp.where(alive, place_ref[first + q], 0)] = jnp.where(
                alive, block, jnp.zeros_like(block)
            )


def renew(side, count, places, keep, other, rotation, total):
    slots, half, width = keep.shape
    new = rotation.shape[1]
    smem = pl.BlockSpec(memory_space=pltpu.SMEM)
    vmem = pl.BlockSpec(memory_space=pltpu.VMEM)
    return pl.pallas_call(
        renew_kernel,
        in_specs=[smem, smem, smem, vmem, vmem, vmem],
        out_specs=vmem,
        out_shape=jax.ShapeDtypeStruct((total, half, new), jnp.bfloat16),
        cost_estimate=pl.CostEstimate(
            flops=2 * slots * half * 2 * width * new,
            bytes_accessed=2 * (2 * slots + total) * half * new,
            transcendentals=0,
        ),
        compiler_params=pltpu.CompilerParams(vmem_limit_bytes=12 * MIB),
        name="renew",
    )(side, count, places, keep, other, rotation)


def sigma_kernel(
    side_ref,
    count_ref,
    wave_ref,
    left_ref,
    right_ref,
    keep_ref,
    send_ref,
    lefts,
    rights,
    total,
    arrived,
):
    slots, rows, cols = lefts.shape
    right = rights.shape[1]
    vectors = wave_ref.shape[0] // cols
    groups = slots // GROUP
    live = count_ref[0]

    def fetch(g):
        part = pl.ds(g * GROUP, GROUP)
        return (
            pltpu.make_async_copy(right_ref.at[part], rights.at[part], arrived.at[0, g]),
            pltpu.make_async_copy(left_ref.at[part], lefts.at[part], arrived.at[1, g]),
        )

    for g in range(groups):
        for copy in fetch(g):
            copy.start()
    total[...] = jnp.zeros_like(total)

    def step(g, carry):
        for copy in fetch(g):
            copy.wait()

        @pl.when(g * GROUP < live)
        def _():
            wave = wave_ref[...]
            alive, products = [], []
            for p in range(GROUP):
                at = g * GROUP + p
                product = lax.dot_general(
                    wave, rights[at], (((1,), (1,)), ((), ())), preferred_element_type=jnp.float32
                ).astype(jnp.bfloat16)
                products.append(product)
                left = lefts[at]
                alive.append(jnp.where(at < live, left, jnp.zeros_like(left)))
            left = jnp.concatenate(alive, axis=1)
            for n in range(vectors):
                stacked = jnp.concatenate([z[n * cols : (n + 1) * cols] for z in products], axis=0)
                term = jnp.dot(left, stacked, preferred_element_type=jnp.float32)
                for c in range(right // LANES):
                    total[n * (right // LANES) + c] += term[:, c * LANES : (c + 1) * LANES]

        return carry

    lax.fori_loop(0, groups, step, 0)
    ring = keep_ref.shape[0]
    span = rows // keep_ref.shape[2]
    side = side_ref[0]
    for z in range(ring):
        for u in range(2):
            at = z * (span // ring) + u
            for c in range(total.shape[0]):
                lanes = slice(c * LANES, (c + 1) * LANES)
                mine = total[c, pl.ds(at + 2 * side, keep_ref.shape[2], stride=span)]
                theirs = total[c, pl.ds(at + 2 - 2 * side, keep_ref.shape[2], stride=span)]
                keep_ref[z, u, :, lanes] = mine
                send_ref[z, u, :, lanes] = theirs.astype(send_ref.dtype)


def apply_pairs(side, count, wave, operators_left, operators_right):
    slots, rows, cols = operators_left.shape
    right = operators_right.shape[1]
    vectors = wave.shape[0] // cols
    part = (4, 2, rows // 16, vectors * right)
    smem = pl.BlockSpec(memory_space=pltpu.SMEM)
    vmem = pl.BlockSpec(memory_space=pltpu.VMEM)
    hbm = pl.BlockSpec(memory_space=pltpu.HBM)
    flops = 2 * slots * (wave.shape[0] * right * right + rows * cols * vectors * right)
    return pl.pallas_call(
        sigma_kernel,
        in_specs=[smem, smem, vmem, hbm, hbm],
        out_specs=[vmem, vmem],
        out_shape=[
            jax.ShapeDtypeStruct(part, jnp.float32),
            jax.ShapeDtypeStruct(part, jnp.bfloat16),
        ],
        scratch_shapes=[
            pltpu.VMEM((slots, rows, cols), jnp.bfloat16),
            pltpu.VMEM((slots, right, right), jnp.bfloat16),
            pltpu.VMEM((vectors * right // LANES, rows, LANES), jnp.float32),
            pltpu.SemaphoreType.DMA((2, slots // GROUP)),
        ],
        cost_estimate=pl.CostEstimate(
            flops=flops,
            bytes_accessed=2 * slots * (rows * cols + right * right),
            transcendentals=0,
        ),
        compiler_params=pltpu.CompilerParams(vmem_limit_bytes=50 * MIB),
        name="apply_pairs",
    )(side, count, wave, operators_left, operators_right)


def store_kernel(in_ref, out_ref, done):
    copy = pltpu.make_async_copy(in_ref, out_ref, done)
    copy.start()
    copy.wait()


def store(x):
    return pl.pallas_call(
        store_kernel,
        in_specs=[pl.BlockSpec(memory_space=pltpu.VMEM)],
        out_specs=pl.BlockSpec(memory_space=pltpu.HBM),
        out_shape=jax.ShapeDtypeStruct(x.shape, x.dtype),
        scratch_shapes=[pltpu.SemaphoreType.DMA],
        cost_estimate=pl.CostEstimate(flops=1 << 22, bytes_accessed=4 * x.size, transcendentals=0),
        compiler_params=pltpu.CompilerParams(vmem_limit_bytes=8 * MIB),
        name="store",
    )(x)


def own_share(blocks, axis):
    size = lax.axis_size(axis)
    me = lax.axis_index(axis)
    parts = []
    for k in range(1, size):
        block = lax.dynamic_index_in_dim(blocks, (me + k) % size, 0, keepdims=False)
        hop = [(i, (i + k) % size) for i in range(size)]
        parts.append(lax.ppermute(block.astype(jnp.bfloat16), axis, hop))
    total = lax.dynamic_index_in_dim(blocks, me, 0, keepdims=False)
    for part in parts:
        total = total + part.astype(jnp.float32)
    return total


def gather_wave(wavefunction):
    cols, vectors, own = wavefunction.shape
    shard = jnp.transpose(wavefunction, (1, 2, 0))
    owners = lax.axis_size(OPS)
    blocks = lax.all_to_all(
        jnp.broadcast_to(shard, (owners, *shard.shape)), OPS, 0, 0, tiled=True
    )
    return jnp.transpose(blocks, (1, 3, 0, 2)).reshape(vectors * cols, owners * own)


def per_device(operators_left, operators_right, wavefunction, rotation, pair_count, next_owner):
    slots, left_states, _ = operators_left.shape
    right_states = operators_right.shape[1]
    vectors = wavefunction.shape[1]
    owners = lax.axis_size(OPS)
    capacity = max(2, 2 * slots // owners)
    side = lax.axis_index("blk").astype(jnp.int32).reshape(1)
    targets = next_owner[:, 0]
    order = lax.iota(jnp.int32, slots)
    same = (targets[:, None] == targets[None, :]) & (order[None, :] < order[:, None])
    places = targets * capacity + jnp.sum(same.astype(jnp.int32), axis=1)

    keep, send = rotate_left(side, operators_left, rotation)
    other = lax.ppermute(send, "blk", [(0, 1), (1, 0)])
    wave = gather_wave(wavefunction)
    outgoing = renew(side, pair_count, places, keep, other, rotation, owners * capacity)
    incoming = lax.all_to_all(outgoing, OPS, split_axis=0, concat_axis=0, tiled=True)
    mine, theirs = apply_pairs(side, pair_count, wave, operators_left, operators_right)
    got = lax.ppermute(theirs, "blk", [(0, 1), (1, 0)])
    mine = own_share(mine + got.astype(jnp.float32), "ops_2")
    parts = jnp.transpose(mine.astype(jnp.bfloat16), (1, 0, 2))
    parts = lax.all_to_all(parts, ("ops_0", "ops_1"), 0, 0, tiled=True)
    renewed = store(incoming)
    sigma = jnp.sum(parts.astype(jnp.float32), axis=0)
    sigma = sigma.reshape(left_states // (2 * owners), vectors, right_states)
    return (sigma, renewed[None])


def solution(mesh):
    split = Mesh(mesh.devices.reshape(4, 4, 4, mesh.shape["blk"]), ALL)
    placed = (
        P(OPS, None, "blk"),
        P(OPS, None, None),
        P("blk", None, OPS),
        P(),
        P(OPS),
        P(OPS, None),
    )
    return jax.shard_map(
        per_device,
        mesh=split,
        in_specs=placed,
        out_specs=(P(ALL, None, None), P(OPS, None, "blk", None)),
        check_vma=False,
    )
```

```python
import jax
import jax.numpy as jnp
from jax import lax
from jax.experimental import pallas as pl
from jax.experimental.pallas import tpu as pltpu
from jax.sharding import Mesh
from jax.sharding import PartitionSpec as P


OPS = ("y", "x_hi", "x_lo", "z")
FIRST = ("x_hi", "z")
LAST = ("x_lo", "y")
ALL = OPS + ("blk",)
GROUP = 8
MIB = 1 << 20
LANES = 128


def rotate_kernel(side_ref, left_ref, rot_ref, keep_ref, send_ref, lefts, turned, arrived):
    slots, half, width = keep_ref.shape
    groups = slots // GROUP

    def fetch(g):
        part = pl.ds(g * GROUP, GROUP)
        return pltpu.make_async_copy(left_ref.at[part], lefts.at[part], arrived.at[g])

    for g in range(groups):
        fetch(g).start()
    own_low = side_ref[0] == 0
    turned[...] = rot_ref[...].T
    rot = turned[...]
    for g in range(groups):
        fetch(g).wait()
        for p in range(g * GROUP, (g + 1) * GROUP, 2):
            both = jnp.concatenate([lefts[p], lefts[p + 1]], axis=1)
            rotated = jnp.dot(rot, both, preferred_element_type=jnp.float32).astype(jnp.bfloat16)
            low, high = rotated[:half], rotated[half:]
            keep = jnp.where(own_low, low, high)
            send = jnp.where(own_low, high, low)
            for q in range(2):
                keep_ref[p + q] = keep[:, q * width : (q + 1) * width]
                send_ref[p + q] = send[:, q * width : (q + 1) * width]


def rotate_left(side, operators_left, rotation):
    slots, rows, cols = operators_left.shape
    new = rotation.shape[1]
    half = jax.ShapeDtypeStruct((slots, new // 2, cols), jnp.bfloat16)
    vmem = pl.BlockSpec(memory_space=pltpu.VMEM)
    return pl.pallas_call(
        rotate_kernel,
        in_specs=[
            pl.BlockSpec(memory_space=pltpu.SMEM),
            pl.BlockSpec(memory_space=pltpu.HBM),
            vmem,
        ],
        out_specs=[vmem, vmem],
        out_shape=[half, half],
        scratch_shapes=[
            pltpu.VMEM((slots, rows, cols), jnp.bfloat16),
            pltpu.VMEM((new, rows), jnp.bfloat16),
            pltpu.SemaphoreType.DMA((slots // GROUP,)),
        ],
        compiler_params=pltpu.CompilerParams(vmem_limit_bytes=50 * MIB),
        cost_estimate=pl.CostEstimate(
            flops=2 * slots * rows * cols * new,
            bytes_accessed=2 * slots * cols * (rows + new),
            transcendentals=0,
        ),
        name="rotate_left",
    )(side, operators_left, rotation)


def renew_kernel(side_ref, count_ref, place_ref, keep_ref, other_ref, rot_ref, out_ref):
    slots, half, width = keep_ref.shape
    live = count_ref[0]
    own_low = side_ref[0] == 0
    top, bottom = rot_ref[:width], rot_ref[width:]
    rot_own = jnp.where(own_low, top, bottom)
    rot_far = jnp.where(own_low, bottom, top)
    rot = jnp.concatenate([rot_own, rot_far], axis=0)
    out_ref[...] = jnp.zeros_like(out_ref)
    for first in range(slots - GROUP, -1, -GROUP):
        w = jnp.concatenate(
            [keep_ref[first : first + GROUP], other_ref[first : first + GROUP]], axis=2
        ).reshape(GROUP * half, 2 * width)
        b = jnp.dot(w, rot, preferred_element_type=jnp.float32).astype(jnp.bfloat16)
        for q in range(GROUP - 1, -1, -1):
            block = b[q * half : (q + 1) * half]
            alive = first + q < live
            out_ref[jnp.where(alive, place_ref[first + q], 0)] = jnp.where(
                alive, block, jnp.zeros_like(block)
            )


def renew(side, count, places, keep, other, rotation, total):
    slots, half, width = keep.shape
    new = rotation.shape[1]
    smem = pl.BlockSpec(memory_space=pltpu.SMEM)
    vmem = pl.BlockSpec(memory_space=pltpu.VMEM)
    return pl.pallas_call(
        renew_kernel,
        in_specs=[smem, smem, smem, vmem, vmem, vmem],
        out_specs=vmem,
        out_shape=jax.ShapeDtypeStruct((total, half, new), jnp.bfloat16),
        cost_estimate=pl.CostEstimate(
            flops=2 * slots * half * 2 * width * new,
            bytes_accessed=2 * (2 * slots + total) * half * new,
            transcendentals=0,
        ),
        compiler_params=pltpu.CompilerParams(vmem_limit_bytes=12 * MIB),
        name="renew",
    )(side, count, places, keep, other, rotation)


def sigma_kernel(
    side_ref,
    count_ref,
    wave_ref,
    left_ref,
    right_ref,
    keep_ref,
    send_ref,
    lefts,
    rights,
    total,
    arrived,
):
    slots, rows, cols = lefts.shape
    right = rights.shape[1]
    vectors = wave_ref.shape[0] // cols
    groups = slots // GROUP
    live = count_ref[0]

    def fetch(g):
        part = pl.ds(g * GROUP, GROUP)
        return (
            pltpu.make_async_copy(right_ref.at[part], rights.at[part], arrived.at[0, g]),
            pltpu.make_async_copy(left_ref.at[part], lefts.at[part], arrived.at[1, g]),
        )

    for g in range(groups):
        for copy in fetch(g):
            copy.start()
    total[...] = jnp.zeros_like(total)

    def step(g, carry):
        for copy in fetch(g):
            copy.wait()

        @pl.when(g * GROUP < live)
        def _():
            wave = wave_ref[...]
            alive, products = [], []
            for p in range(GROUP):
                at = g * GROUP + p
                product = lax.dot_general(
                    wave, rights[at], (((1,), (1,)), ((), ())), preferred_element_type=jnp.float32
                ).astype(jnp.bfloat16)
                products.append(product)
                left = lefts[at]
                alive.append(jnp.where(at < live, left, jnp.zeros_like(left)))
            left = jnp.concatenate(alive, axis=1)
            for n in range(vectors):
                stacked = jnp.concatenate([z[n * cols : (n + 1) * cols] for z in products], axis=0)
                term = jnp.dot(left, stacked, preferred_element_type=jnp.float32)
                for c in range(right // LANES):
                    total[n * (right // LANES) + c] += term[:, c * LANES : (c + 1) * LANES]

        return carry

    lax.fori_loop(0, groups, step, 0)
    side = side_ref[0]
    outer = keep_ref.shape[2] // 2
    span = rows // outer
    ring = keep_ref.shape[0] // 2
    unit = span // (4 * ring)
    for group in range(2 * ring):
        for u in range(2):
            at = (group // ring * 2 * ring + group % ring) * unit + u
            for c in range(total.shape[0]):
                lanes = slice(c * LANES, (c + 1) * LANES)

                def lines(half):
                    return jnp.concatenate(
                        [
                            total[c, pl.ds(at + low * ring * unit + 2 * half, outer, stride=span)]
                            for low in range(2)
                        ],
                        axis=0,
                    )

                keep_ref[group, u, :, lanes] = lines(side)
                send_ref[group, u, :, lanes] = lines(1 - side).astype(send_ref.dtype)


def apply_pairs(near, side, count, wave, operators_left, operators_right):
    slots, rows, cols = operators_left.shape
    right = operators_right.shape[1]
    vectors = wave.shape[0] // cols
    part = (near, 2, rows // (4 * near), vectors * right)
    smem = pl.BlockSpec(memory_space=pltpu.SMEM)
    vmem = pl.BlockSpec(memory_space=pltpu.VMEM)
    hbm = pl.BlockSpec(memory_space=pltpu.HBM)
    flops = 2 * slots * (wave.shape[0] * right * right + rows * cols * vectors * right)
    return pl.pallas_call(
        sigma_kernel,
        in_specs=[smem, smem, vmem, hbm, hbm],
        out_specs=[vmem, vmem],
        out_shape=[
            jax.ShapeDtypeStruct(part, jnp.float32),
            jax.ShapeDtypeStruct(part, jnp.bfloat16),
        ],
        scratch_shapes=[
            pltpu.VMEM((slots, rows, cols), jnp.bfloat16),
            pltpu.VMEM((slots, right, right), jnp.bfloat16),
            pltpu.VMEM((vectors * right // LANES, rows, LANES), jnp.float32),
            pltpu.SemaphoreType.DMA((2, slots // GROUP)),
        ],
        cost_estimate=pl.CostEstimate(
            flops=flops,
            bytes_accessed=2 * slots * (rows * cols + right * right),
            transcendentals=0,
        ),
        compiler_params=pltpu.CompilerParams(vmem_limit_bytes=50 * MIB),
        name="apply_pairs",
    )(side, count, wave, operators_left, operators_right)


def store_kernel(in_ref, out_ref, done):
    copy = pltpu.make_async_copy(in_ref, out_ref, done)
    copy.start()
    copy.wait()


def store(x):
    return pl.pallas_call(
        store_kernel,
        in_specs=[pl.BlockSpec(memory_space=pltpu.VMEM)],
        out_specs=pl.BlockSpec(memory_space=pltpu.HBM),
        out_shape=jax.ShapeDtypeStruct(x.shape, x.dtype),
        scratch_shapes=[pltpu.SemaphoreType.DMA],
        cost_estimate=pl.CostEstimate(flops=1 << 22, bytes_accessed=4 * x.size, transcendentals=0),
        compiler_params=pltpu.CompilerParams(vmem_limit_bytes=8 * MIB),
        name="store",
    )(x)


def own_share(blocks, axes):
    first, second = (lax.axis_size(axis) for axis in axes)
    here = [lax.axis_index(axis) for axis in axes]
    own = here[0] * second + here[1]
    parts = []
    for k in range(1, first * second):
        far, near = k // second, k % second

        def target(i, j):
            return (i + far) % first * second + (j + near) % second

        hop = [(i * second + j, target(i, j)) for i in range(first) for j in range(second)]
        block = lax.dynamic_index_in_dim(blocks, target(*here), 0, keepdims=False)
        parts.append(lax.ppermute(block.astype(jnp.bfloat16), axes, hop))
    total = lax.dynamic_index_in_dim(blocks, own, 0, keepdims=False)
    for part in parts:
        total = total + part.astype(jnp.float32)
    return total


def gather_wave(wavefunction):
    cols, vectors, own = wavefunction.shape
    shard = jnp.transpose(wavefunction, (1, 2, 0))
    owners = lax.axis_size(OPS)
    blocks = lax.all_to_all(
        jnp.broadcast_to(shard, (owners, *shard.shape)), OPS, 0, 0, tiled=True
    )
    return jnp.transpose(blocks, (1, 3, 0, 2)).reshape(vectors * cols, owners * own)


def per_device(operators_left, operators_right, wavefunction, rotation, pair_count, next_owner):
    slots, left_states, _ = operators_left.shape
    right_states = operators_right.shape[1]
    vectors = wavefunction.shape[1]
    owners = lax.axis_size(OPS)
    capacity = max(2, 2 * slots // owners)
    side = lax.axis_index("blk").astype(jnp.int32).reshape(1)
    targets = next_owner[:, 0]
    order = lax.iota(jnp.int32, slots)
    same = (targets[:, None] == targets[None, :]) & (order[None, :] < order[:, None])
    places = targets * capacity + jnp.sum(same.astype(jnp.int32), axis=1)

    keep, send = rotate_left(side, operators_left, rotation)
    other = lax.ppermute(send, "blk", [(0, 1), (1, 0)])
    wave = gather_wave(wavefunction)
    outgoing = renew(side, pair_count, places, keep, other, rotation, owners * capacity)
    incoming = lax.all_to_all(outgoing, OPS, split_axis=0, concat_axis=0, tiled=True)
    mine, theirs = apply_pairs(lax.axis_size(FIRST), side, pair_count, wave, operators_left, operators_right)
    got = lax.ppermute(theirs, "blk", [(0, 1), (1, 0)])
    mine = own_share(mine + got.astype(jnp.float32), FIRST)
    parts = jnp.transpose(mine.astype(jnp.bfloat16), (1, 0, 2))
    parts = lax.all_to_all(parts, LAST, 0, 0, tiled=True)
    renewed = store(incoming)
    sigma = jnp.sum(parts.astype(jnp.float32), axis=0)
    sigma = sigma.reshape(left_states // (2 * owners), vectors, right_states)
    return (sigma, renewed[None])


def solution(mesh):
    split = Mesh(mesh.devices.reshape(4, 2, 2, 4, mesh.shape["blk"]), ALL)
    placed = (
        P(OPS, None, "blk"),
        P(OPS, None, None),
        P("blk", None, OPS),
        P(),
        P(OPS),
        P(OPS, None),
    )
    return jax.shard_map(
        per_device,
        mesh=split,
        in_specs=placed,
        out_specs=(P(ALL, None, None), P(OPS, None, "blk", None)),
        check_vma=False,
    )
```

```python
import functools

import jax
import jax.numpy as jnp
from jax import lax
from jax.experimental import pallas as pl
from jax.experimental.pallas import tpu as pltpu
from jax.sharding import Mesh
from jax.sharding import PartitionSpec as P


OPS = ("y", "x_hi", "x_lo", "z")
FIRST = ("x_hi", "z")
LAST = ("x_lo", "y")
ALL = OPS + ("blk",)
GROUP = 8
MIB = 1 << 20
LANES = 128


def rotate_kernel(start, side_ref, left_ref, rot_ref, keep_ref, send_ref, lefts, turned, arrived):
    slots, half, width = keep_ref.shape
    groups = slots // GROUP

    def fetch(g):
        part = pl.ds(g * GROUP, GROUP)
        there = pl.ds(start + g * GROUP, GROUP)
        return pltpu.make_async_copy(left_ref.at[there], lefts.at[part], arrived.at[g])

    for g in range(groups):
        fetch(g).start()
    own_low = side_ref[0] == 0
    turned[...] = rot_ref[...].T
    rot = turned[...]
    for g in range(groups):
        fetch(g).wait()
        for p in range(g * GROUP, (g + 1) * GROUP, 2):
            both = jnp.concatenate([lefts[p], lefts[p + 1]], axis=1)
            rotated = jnp.dot(rot, both, preferred_element_type=jnp.float32).astype(jnp.bfloat16)
            low, high = rotated[:half], rotated[half:]
            keep = jnp.where(own_low, low, high)
            send = jnp.where(own_low, high, low)
            for q in range(2):
                keep_ref[p + q] = keep[:, q * width : (q + 1) * width]
                send_ref[p + q] = send[:, q * width : (q + 1) * width]


def rotate_left(side, operators_left, rotation, start, slots):
    _, rows, cols = operators_left.shape
    new = rotation.shape[1]
    half = jax.ShapeDtypeStruct((slots, new // 2, cols), jnp.bfloat16)
    vmem = pl.BlockSpec(memory_space=pltpu.VMEM)
    return pl.pallas_call(
        functools.partial(rotate_kernel, start),
        in_specs=[
            pl.BlockSpec(memory_space=pltpu.SMEM),
            pl.BlockSpec(memory_space=pltpu.HBM),
            vmem,
        ],
        out_specs=[vmem, vmem],
        out_shape=[half, half],
        scratch_shapes=[
            pltpu.VMEM((slots, rows, cols), jnp.bfloat16),
            pltpu.VMEM((new, rows), jnp.bfloat16),
            pltpu.SemaphoreType.DMA((slots // GROUP,)),
        ],
        compiler_params=pltpu.CompilerParams(vmem_limit_bytes=50 * MIB),
        cost_estimate=pl.CostEstimate(
            flops=2 * slots * rows * cols * new,
            bytes_accessed=2 * slots * cols * (rows + new),
            transcendentals=0,
        ),
        name="rotate_left",
    )(side, operators_left, rotation)


def renew_kernel(side_ref, count_ref, place_ref, rot_ref, *refs):
    *pieces, out_ref = refs
    keeps, others = pieces[: len(pieces) // 2], pieces[len(pieces) // 2 :]
    piece, half, width = keeps[0].shape
    slots = piece * len(keeps)
    live = count_ref[0]
    own_low = side_ref[0] == 0
    top, bottom = rot_ref[:width], rot_ref[width:]
    rot_own = jnp.where(own_low, top, bottom)
    rot_far = jnp.where(own_low, bottom, top)
    rot = jnp.concatenate([rot_own, rot_far], axis=0)
    out_ref[...] = jnp.zeros_like(out_ref)
    for first in range(slots - GROUP, -1, -GROUP):
        group = slice(first % piece, first % piece + GROUP)
        w = jnp.concatenate(
            [keeps[first // piece][group], others[first // piece][group]], axis=2
        ).reshape(GROUP * half, 2 * width)
        b = jnp.dot(w, rot, preferred_element_type=jnp.float32).astype(jnp.bfloat16)
        for q in range(GROUP - 1, -1, -1):
            block = b[q * half : (q + 1) * half]
            alive = first + q < live
            out_ref[jnp.where(alive, place_ref[first + q], 0)] = jnp.where(
                alive, block, jnp.zeros_like(block)
            )


def renew(side, count, places, keeps, others, rotation, total):
    piece, half, width = keeps[0].shape
    slots = piece * len(keeps)
    new = rotation.shape[1]
    smem = pl.BlockSpec(memory_space=pltpu.SMEM)
    vmem = pl.BlockSpec(memory_space=pltpu.VMEM)
    return pl.pallas_call(
        renew_kernel,
        in_specs=[smem, smem, smem] + [vmem] * (1 + 2 * len(keeps)),
        out_specs=vmem,
        out_shape=jax.ShapeDtypeStruct((total, half, new), jnp.bfloat16),
        cost_estimate=pl.CostEstimate(
            flops=2 * slots * half * 2 * width * new,
            bytes_accessed=2 * (2 * slots + total) * half * new,
            transcendentals=0,
        ),
        compiler_params=pltpu.CompilerParams(vmem_limit_bytes=12 * MIB),
        name="renew",
    )(side, count, places, rotation, *keeps, *others)


def sigma_kernel(
    side_ref,
    count_ref,
    wave_ref,
    left_ref,
    right_ref,
    keep_ref,
    send_ref,
    lefts,
    rights,
    total,
    arrived,
):
    slots, rows, cols = lefts.shape
    right = rights.shape[1]
    vectors = wave_ref.shape[0] // cols
    groups = slots // GROUP
    live = count_ref[0]

    def fetch(g):
        part = pl.ds(g * GROUP, GROUP)
        return (
            pltpu.make_async_copy(right_ref.at[part], rights.at[part], arrived.at[0, g]),
            pltpu.make_async_copy(left_ref.at[part], lefts.at[part], arrived.at[1, g]),
        )

    for g in range(groups):
        for copy in fetch(g):
            copy.start()
    total[...] = jnp.zeros_like(total)

    def step(g, carry):
        for copy in fetch(g):
            copy.wait()

        @pl.when(g * GROUP < live)
        def _():
            wave = wave_ref[...]
            alive, products = [], []
            for p in range(GROUP):
                at = g * GROUP + p
                product = lax.dot_general(
                    wave, rights[at], (((1,), (1,)), ((), ())), preferred_element_type=jnp.float32
                ).astype(jnp.bfloat16)
                products.append(product)
                left = lefts[at]
                alive.append(jnp.where(at < live, left, jnp.zeros_like(left)))
            left = jnp.concatenate(alive, axis=1)
            for n in range(vectors):
                stacked = jnp.concatenate([z[n * cols : (n + 1) * cols] for z in products], axis=0)
                term = jnp.dot(left, stacked, preferred_element_type=jnp.float32)
                for c in range(right // LANES):
                    total[n * (right // LANES) + c] += term[:, c * LANES : (c + 1) * LANES]

        return carry

    lax.fori_loop(0, groups, step, 0)
    side = side_ref[0]
    outer = keep_ref.shape[2] // 2
    span = rows // outer
    ring = keep_ref.shape[0] // 2
    unit = span // (4 * ring)
    for group in range(2 * ring):
        for u in range(2):
            at = (group // ring * 2 * ring + group % ring) * unit + u
            for c in range(total.shape[0]):
                lanes = slice(c * LANES, (c + 1) * LANES)

                def lines(half):
                    return jnp.concatenate(
                        [
                            total[c, pl.ds(at + low * ring * unit + 2 * half, outer, stride=span)]
                            for low in range(2)
                        ],
                        axis=0,
                    )

                keep_ref[group, u, :, lanes] = lines(side)
                send_ref[group, u, :, lanes] = lines(1 - side).astype(send_ref.dtype)


def apply_pairs(near, side, count, wave, operators_left, operators_right):
    slots, rows, cols = operators_left.shape
    right = operators_right.shape[1]
    vectors = wave.shape[0] // cols
    part = (near, 2, rows // (4 * near), vectors * right)
    smem = pl.BlockSpec(memory_space=pltpu.SMEM)
    vmem = pl.BlockSpec(memory_space=pltpu.VMEM)
    hbm = pl.BlockSpec(memory_space=pltpu.HBM)
    flops = 2 * slots * (wave.shape[0] * right * right + rows * cols * vectors * right)
    return pl.pallas_call(
        sigma_kernel,
        in_specs=[smem, smem, vmem, hbm, hbm],
        out_specs=[vmem, vmem],
        out_shape=[
            jax.ShapeDtypeStruct(part, jnp.float32),
            jax.ShapeDtypeStruct(part, jnp.bfloat16),
        ],
        scratch_shapes=[
            pltpu.VMEM((slots, rows, cols), jnp.bfloat16),
            pltpu.VMEM((slots, right, right), jnp.bfloat16),
            pltpu.VMEM((vectors * right // LANES, rows, LANES), jnp.float32),
            pltpu.SemaphoreType.DMA((2, slots // GROUP)),
        ],
        cost_estimate=pl.CostEstimate(
            flops=flops,
            bytes_accessed=2 * slots * (rows * cols + right * right),
            transcendentals=0,
        ),
        compiler_params=pltpu.CompilerParams(vmem_limit_bytes=50 * MIB),
        name="apply_pairs",
    )(side, count, wave, operators_left, operators_right)


def store_kernel(in_ref, out_ref, done):
    copy = pltpu.make_async_copy(in_ref, out_ref, done)
    copy.start()
    copy.wait()


def store(x):
    return pl.pallas_call(
        store_kernel,
        in_specs=[pl.BlockSpec(memory_space=pltpu.VMEM)],
        out_specs=pl.BlockSpec(memory_space=pltpu.HBM),
        out_shape=jax.ShapeDtypeStruct(x.shape, x.dtype),
        scratch_shapes=[pltpu.SemaphoreType.DMA],
        cost_estimate=pl.CostEstimate(flops=1 << 22, bytes_accessed=4 * x.size, transcendentals=0),
        compiler_params=pltpu.CompilerParams(vmem_limit_bytes=8 * MIB),
        name="store",
    )(x)


def own_share(blocks, axes):
    first, second = (lax.axis_size(axis) for axis in axes)
    here = [lax.axis_index(axis) for axis in axes]
    own = here[0] * second + here[1]
    parts = []
    for k in range(1, first * second):
        far, near = k // second, k % second

        def target(i, j):
            return (i + far) % first * second + (j + near) % second

        hop = [(i * second + j, target(i, j)) for i in range(first) for j in range(second)]
        block = lax.dynamic_index_in_dim(blocks, target(*here), 0, keepdims=False)
        parts.append(lax.ppermute(block.astype(jnp.bfloat16), axes, hop))
    total = lax.dynamic_index_in_dim(blocks, own, 0, keepdims=False)
    for part in parts:
        total = total + part.astype(jnp.float32)
    return total


def gather_wave(wavefunction):
    cols, vectors, own = wavefunction.shape
    shard = jnp.transpose(wavefunction, (1, 2, 0))
    owners = lax.axis_size(OPS)
    blocks = lax.all_to_all(
        jnp.broadcast_to(shard, (owners, *shard.shape)), OPS, 0, 0, tiled=True
    )
    return jnp.transpose(blocks, (1, 3, 0, 2)).reshape(vectors * cols, owners * own)


def per_device(operators_left, operators_right, wavefunction, rotation, pair_count, next_owner):
    slots, left_states, _ = operators_left.shape
    right_states = operators_right.shape[1]
    vectors = wavefunction.shape[1]
    owners = lax.axis_size(OPS)
    capacity = max(2, 2 * slots // owners)
    side = lax.axis_index("blk").astype(jnp.int32).reshape(1)
    targets = next_owner[:, 0]
    order = lax.iota(jnp.int32, slots)
    same = (targets[:, None] == targets[None, :]) & (order[None, :] < order[:, None])
    places = targets * capacity + jnp.sum(same.astype(jnp.int32), axis=1)

    keeps, others = [], []
    for start in range(0, slots, slots // 2):
        keep, send = rotate_left(side, operators_left, rotation, start, slots // 2)
        others.append(lax.ppermute(send, "blk", [(0, 1), (1, 0)]))
        keeps.append(keep)
    wave = gather_wave(wavefunction)
    outgoing = renew(side, pair_count, places, keeps, others, rotation, owners * capacity)
    incoming = lax.all_to_all(outgoing, OPS, split_axis=0, concat_axis=0, tiled=True)
    mine, theirs = apply_pairs(lax.axis_size(FIRST), side, pair_count, wave, operators_left, operators_right)
    got = lax.ppermute(theirs, "blk", [(0, 1), (1, 0)])
    mine = own_share(mine + got.astype(jnp.float32), FIRST)
    parts = jnp.transpose(mine.astype(jnp.bfloat16), (1, 0, 2))
    parts = lax.all_to_all(parts, LAST, 0, 0, tiled=True)
    renewed = store(incoming)
    sigma = jnp.sum(parts.astype(jnp.float32), axis=0)
    sigma = sigma.reshape(left_states // (2 * owners), vectors, right_states)
    return (sigma, renewed[None])


def solution(mesh):
    split = Mesh(mesh.devices.reshape(4, 2, 2, 4, mesh.shape["blk"]), ALL)
    placed = (
        P(OPS, None, "blk"),
        P(OPS, None, None),
        P("blk", None, OPS),
        P(),
        P(OPS),
        P(OPS, None),
    )
    return jax.shard_map(
        per_device,
        mesh=split,
        in_specs=placed,
        out_specs=(P(ALL, None, None), P(OPS, None, "blk", None)),
        check_vma=False,
    )
```
